32 devices in a mesh: grow: 8 (over y, x, core), gcol: 4 (over z).
Axes of the slice: x: 2, y: 2, z: 4, core: 2. Of those that a mesh axis runs over, the one named last changes fastest.
Arguments:
- eps_static: float32 [12288, 12288], P('grow', 'gcol'), may hold values from -1.8 to 1.8
- eps_imag: float32 [12288, 12288], P('grow', 'gcol'), may hold values from -1.8 to 1.8
- frequency_grid: float32 [3], replicated, may hold values from 0.1 to 2
- band_energy: float32 [32], replicated, may hold values from -2 to 2
- pair_elements: bfloat16 [32, 64, 12288], P('grow', None, 'gcol'), may hold values from -0.0546875 to 0.0546875
Outputs:
- sigma: float32 [3, 64], P(None, 'gcol')
The draws below stay inside these ranges and needn't reach their ends.
All inputs are finite; a program needn't handle non-finite values.
Results may differ from the reference program's by a relative error of at most 0.0019.
Values may be sent and summed in bfloat16 or wider, within the bound.
A program may use at most 128 MiB of HBM per device.

```python
import math
import jax
import jax.numpy as jnp
from jax import lax

NG = 12288
STATES = 64
BANDS = 32
NE = 3


def block_levels(key, extent, cuts, low, high):
    level, own = 1.0, jax.random.fold_in(key, 6)
    for position, parts in cuts:
        heights = jnp.exp(jax.random.uniform(jax.random.fold_in(own, position), (parts,), jnp.float32, low / len(cuts), high / len(cuts)))
        level = level * jnp.repeat(heights, extent[position] // parts).reshape([-1 if axis == position else 1 for axis in range(len(extent))])
    return level


def gaussian(own_key, dims, scale, limit, cuts=(), kind=jnp.bfloat16):
    entries = scale * jax.random.normal(own_key, dims, jnp.float32)
    if cuts:
        entries = entries * block_levels(own_key, dims, cuts, -0.22, 0.18)
    return jnp.clip(entries, -limit, limit).astype(kind)


def setup_inputs(seed: int = 0) -> dict:
    arg_keys = jax.random.split(jax.random.key(seed), 6)
    eps_static = gaussian(arg_keys[0], (NG, NG), 0.3, 1.8, ((0, 8), (1, 4)), jnp.float32)
    eps_imag = gaussian(arg_keys[1], (NG, NG), 0.3, 1.8, ((0, 8), (1, 4)), jnp.float32)
    frequency_grid = jnp.clip(jnp.exp(jax.random.uniform(arg_keys[2], (NE,), jnp.float32, math.log(0.1), math.log(2.0))), 0.1, 2.0)
    band_energy = jnp.clip(jax.random.uniform(arg_keys[3], (BANDS,), jnp.float32, -2.0, 2.0), -2.0, 2.0)
    pair_elements = gaussian(arg_keys[4], (BANDS, STATES, NG), NG ** -0.5, 0.0546875, ((0, 8), (2, 4)))
    return dict(eps_static=eps_static, eps_imag=eps_imag, frequency_grid=frequency_grid, band_energy=band_energy, pair_elements=pair_elements)


def pole_kernels(static_rows, imag_rows, kronecker, frequency_grid):
    static_part = static_rows - kronecker
    imag_part = imag_rows - kronecker
    spread = static_part - imag_part
    pole_square = (imag_part * imag_part + 0.25) / (spread * spread + 0.25)
    pole_freq = jnp.sqrt(pole_square)
    strength = -static_part * pole_square
    return [(strength / (pole_freq * (pole_freq + frequency_grid[point]))).astype(jnp.bfloat16) for point in range(NE)]

def reference(eps_static, eps_imag, frequency_grid, band_energy, pair_elements):
    blocks = 16
    height = NG // blocks
    rows_all = pair_elements.reshape(BANDS * STATES, NG).astype(jnp.float32)
    col_ids = lax.iota(jnp.int32, NG)
    row_ids = lax.iota(jnp.int32, height)

    def advance(block, quad):
        start = (block * height).astype(jnp.int32)
        static_rows = lax.dynamic_slice_in_dim(eps_static, start, height, 0)
        imag_rows = lax.dynamic_slice_in_dim(eps_imag, start, height, 0)
        kronecker = ((start + row_ids)[:, None] == col_ids[None, :]).astype(jnp.float32)
        kernels = pole_kernels(static_rows, imag_rows, kronecker, frequency_grid)
        left = lax.dynamic_slice_in_dim(rows_all, start, height, 1)
        terms = []
        for kernel in kernels:
            wide = lax.optimization_barrier(kernel).astype(jnp.float32)
            projected = jnp.dot(left, wide, precision=lax.Precision.HIGHEST)
            terms.append(lax.optimization_barrier(jnp.sum(projected * rows_all, axis=1)))
        return quad + jnp.stack(terms)
    quad = lax.fori_loop(0, blocks, advance, jnp.zeros((NE, BANDS * STATES), jnp.float32))
    quad = quad.reshape(NE, BANDS, STATES)
    offset = frequency_grid[:, None] - band_energy[None, :]
    weight = 1.0 / (1.0 + offset * offset)
    return jnp.einsum('em,ems->es', weight, quad)
```

```python
import functools

import jax
import jax.numpy as jnp
from jax import lax
from jax.experimental import pallas as pl
from jax.experimental.pallas import tpu as pltpu
from jax.sharding import PartitionSpec as P

LANES = 128
SUB_ROWS = 32
SUB_COLS = 512
DOT_COLS = 256


def bit_flip(index, mask, extent):
    total, bit = 0, 1
    while bit < extent:
        total = total + ((index // bit + mask // bit) % 2) * bit
        bit *= 2
    return total


def body(R, Z, bpd, states, height, breadth, ne,
         freq, energy, es_hbm, ei_hbm, pair_hbm, out,
         kern, colp, rowp, es_buf, ei_buf, sig, part, recv1, recv2,
         eps_sem, own_sem, col_send, col_recv, row_recv, up_send, dn_send,
         s1_send, s1_recv, s2_send, s2_recv):
    r = lax.axis_index("grow")
    z = lax.axis_index("gcol")
    ratio = R // Z
    home = r // ratio
    offset = pl.multiple_of(r % ratio * height, height)
    spc = states // Z
    units = R * bpd
    blocks = 4 * bpd
    rows = height // blocks

    def dev(row, col):
        return dict(device_id={"grow": row, "gcol": col}, device_id_type=pl.DeviceIdType.MESH)

    def eps_copies(block, slot):
        at = pl.multiple_of(block * rows, rows)
        return (pltpu.make_async_copy(es_hbm.at[pl.ds(at, rows), :], es_buf.at[slot], eps_sem.at[0, slot]),
                pltpu.make_async_copy(ei_hbm.at[pl.ds(at, rows), :], ei_buf.at[slot], eps_sem.at[1, slot]))

    own = pltpu.make_async_copy(pair_hbm, colp.at[0], own_sem)
    own.start()
    for copy in eps_copies(0, 0):
        copy.start()

    barrier = pltpu.get_barrier_semaphore()
    for d in range(1, R):
        pl.semaphore_signal(barrier, inc=1, **dev((r + d) % R, z))
    for d in range(1, Z):
        pl.semaphore_signal(barrier, inc=1, **dev(r, (z + d) % Z))
    sig[...] = jnp.zeros_like(sig)
    own.wait()
    pl.semaphore_wait(barrier, R + Z - 2)

    def unit_rows(b):
        return pl.ds(pl.multiple_of(b * states, states), states)

    def col_copy(src_shard, dst_shard, b, row):
        return pltpu.make_async_remote_copy(
            src_ref=colp.at[src_shard, unit_rows(b), :], dst_ref=colp.at[dst_shard, unit_rows(b), :],
            send_sem=col_send.at[dst_shard * bpd + b], recv_sem=col_recv.at[dst_shard * bpd + b],
            **dev(row, z))

    partner = bit_flip(r, 1, R)

    def send_own(b, carry):
        col_copy(0, 1, b, partner).start()
        return carry
    lax.fori_loop(0, bpd, send_own, 0)
    for shard in range(2, R, 2):
        peer = bit_flip(r, shard, R)

        def send_far(b, carry, shard=shard, peer=peer):
            col_copy(0, shard, b, peer).start()
            return carry
        lax.fori_loop(0, bpd, send_far, 0)

    def row_copy(shard, b, u, sems, col):
        ref = rowp.at[shard, unit_rows(b), :]
        return pltpu.make_async_remote_copy(
            src_ref=ref, dst_ref=ref, send_sem=sems.at[u], recv_sem=row_recv.at[u], **dev(r, col))

    goes_up = jnp.logical_and(z >= home, z < Z - 1)
    goes_down = jnp.logical_and(z <= home, z > 0)
    upper = (z + 1) % Z
    lower = (z + Z - 1) % Z

    def comm(u):
        shard, b = u // bpd, u % bpd

        @pl.when(shard >= 1)
        def _():
            col_copy(0, shard, b, partner).wait_recv()

        @pl.when(jnp.logical_and(shard >= 2, shard % 2 == 0))
        def _():
            col_copy(shard, shard + 1, b, partner).start()

        @pl.when(z == home)
        def _():
            local = pltpu.make_async_copy(
                colp.at[shard, unit_rows(b), pl.ds(offset, height)],
                rowp.at[shard, unit_rows(b), :], row_recv.at[u])
            local.start()
            local.wait()

        @pl.when(z != home)
        def _():
            row_copy(shard, b, u, up_send, upper).wait_recv()

        @pl.when(goes_up)
        def _():
            row_copy(shard, b, u, up_send, upper).start()

        @pl.when(goes_down)
        def _():
            row_copy(shard, b, u, dn_send, lower).start()

    diagonal = r * height - z * breadth
    sub_rows = min(SUB_ROWS, rows)
    sub_cols = min(SUB_COLS, breadth)
    col_steps = breadth // sub_cols
    f0, f1, f2 = freq[0], freq[1], freq[2]

    def make_block(block):
        slot = block % 2

        @pl.when(block + 1 < blocks)
        def _():
            for copy in eps_copies(block + 1, 1 - slot):
                copy.start()
        for copy in eps_copies(block, slot):
            copy.wait()
        base = pl.multiple_of(block * rows, rows)

        def chunk(n, carry):
            at_row = pl.multiple_of(n // col_steps * sub_rows, sub_rows)
            at_col = pl.multiple_of(n % col_steps * sub_cols, sub_cols)
            where = (pl.ds(at_row, sub_rows), pl.ds(at_col, sub_cols))
            gap = (lax.broadcasted_iota(jnp.int32, (sub_rows, sub_cols), 0)
                   - lax.broadcasted_iota(jnp.int32, (sub_rows, sub_cols), 1))
            one = jnp.where(gap == at_col - at_row - base - diagonal, 1.0, 0.0)
            static = es_buf[(slot,) + where] - one
            imag = ei_buf[(slot,) + where] - one
            spread = static - imag
            over = imag * imag + 0.25
            under = spread * spread + 0.25
            pole = over * lax.rsqrt(over * under)
            p0, p1, p2 = pole + f0, pole + f1, pole + f2
            p01 = p0 * p1
            scale = -static * pole / (p01 * p2)
            to = (pl.ds(pl.multiple_of(base + at_row, sub_rows), sub_rows), where[1])
            kern[(0,) + to] = (p1 * p2 * scale).astype(jnp.bfloat16)
            kern[(1,) + to] = (p0 * p2 * scale).astype(jnp.bfloat16)
            kern[(2,) + to] = (p01 * scale).astype(jnp.bfloat16)
            return carry
        lax.fori_loop(0, rows // sub_rows * col_steps, chunk, 0)

    width = breadth // bpd
    dot_cols = min(DOT_COLS, width)
    while width % dot_cols:
        dot_cols //= 2

    def piece(number):
        shard, q = number // bpd, number % bpd
        first = bit_flip(r, shard, R) * bpd

        def step(n, carry):
            cols = pl.ds(pl.multiple_of(q * width + n * dot_cols, dot_cols), dot_cols)
            right = colp[shard, :, cols].astype(jnp.float32)
            left = rowp[shard]
            sums = []
            for e in range(ne):
                prod = jnp.dot(left, kern[e, :, cols], preferred_element_type=jnp.float32) * right
                thin = prod[:, :LANES]
                for k in range(1, dot_cols // LANES):
                    thin = thin + prod[:, k * LANES:(k + 1) * LANES]
                total = carry[e]
                for b in range(bpd):
                    miss = jnp.full((8, LANES), freq[e] - energy[first + b], jnp.float32)
                    weight = (1.0 / (1.0 + miss * miss))[:1]
                    total = total + weight * thin[b * states:(b + 1) * states]
                sums.append(total)
            return tuple(sums)
        start = tuple(sig[e] for e in range(ne))
        done = lax.fori_loop(0, width // dot_cols, step, start)
        for e in range(ne):
            sig[e] = done[e]

    def phase_a(u, carry):
        comm(u)
        make_block(2 * u)
        make_block(2 * u + 1)
        return carry
    lax.fori_loop(0, 2 * bpd, phase_a, 0)

    def phase_b(u, carry):
        comm(u)
        piece(2 * (u - 2 * bpd))
        piece(2 * (u - 2 * bpd) + 1)
        return carry
    lax.fori_loop(2 * bpd, 3 * bpd, phase_b, 0)

    def phase_c(u, carry):
        comm(u)
        piece(u - bpd)
        return carry
    lax.fori_loop(3 * bpd, units, phase_c, 0)

    def phase_d(u, carry):
        piece(u - bpd)
        return carry
    lax.fori_loop(units, units + bpd, phase_d, 0)

    for owner in range(Z):
        for e in range(ne):
            part[owner, e] = sig[e, owner * spc:(owner + 1) * spc]

    def s1_copy(d):
        return pltpu.make_async_remote_copy(
            src_ref=part.at[(z + d) % Z], dst_ref=recv1.at[d - 1],
            send_sem=s1_send.at[d - 1], recv_sem=s1_recv.at[d - 1], **dev(r, (z + d) % Z))

    def s2_copy(d, owner):
        return pltpu.make_async_remote_copy(
            src_ref=recv2.at[owner], dst_ref=recv2.at[owner],
            send_sem=s2_send.at[d - 1], recv_sem=s2_recv.at[owner], **dev((r + d) % R, z))

    for d in range(1, Z):
        s1_copy(d).start()

    def drain(u, carry):
        shard, b = u // bpd, u % bpd

        @pl.when(shard >= 1)
        def _():
            col_copy(0, shard, b, partner).wait_send()

        @pl.when(goes_up)
        def _():
            row_copy(shard, b, u, up_send, upper).wait_send()

        @pl.when(goes_down)
        def _():
            row_copy(shard, b, u, dn_send, lower).wait_send()
        return carry
    lax.fori_loop(0, units, drain, 0)

    mine = part[z]
    for d in range(1, Z):
        s1_copy(d).wait_recv()
        mine = mine + recv1[d - 1]
    recv2[r] = mine
    for d in range(1, R):
        s2_copy(d, r).start()
    for d in range(1, R):
        s2_copy(d, (r + R - d) % R).wait_recv()
    full = recv2[0]
    for owner in range(1, R):
        full = full + recv2[owner]
    out[...] = jnp.sum(full, axis=-1)
    for d in range(1, Z):
        s1_copy(d).wait_send()
    for d in range(1, R):
        s2_copy(d, r).wait_send()


def solution(mesh):
    R, Z = mesh.shape["grow"], mesh.shape["gcol"]

    def shards(eps_static, eps_imag, frequency_grid, band_energy, pair_elements):
        height, breadth = eps_static.shape
        bpd, states, _ = pair_elements.shape
        ne = frequency_grid.shape[0]
        spc = states // Z
        rows = height // (4 * bpd)
        dma = pltpu.SemaphoreType.DMA
        units = R * bpd
        any_space = pl.BlockSpec(memory_space=pl.ANY)
        smem = pl.BlockSpec(memory_space=pltpu.SMEM)
        return pl.pallas_call(
            functools.partial(body, R, Z, bpd, states, height, breadth, ne),
            out_shape=jax.ShapeDtypeStruct((ne, spc), jnp.float32),
            in_specs=[smem, smem, any_space, any_space, any_space],
            out_specs=pl.BlockSpec(memory_space=pltpu.VMEM),
            scratch_shapes=[
                pltpu.VMEM((ne, height, breadth), jnp.bfloat16),
                pltpu.VMEM((R, bpd * states, breadth), jnp.bfloat16),
                pltpu.VMEM((R, bpd * states, height), jnp.bfloat16),
                pltpu.VMEM((2, rows, breadth), jnp.float32),
                pltpu.VMEM((2, rows, breadth), jnp.float32),
                pltpu.VMEM((ne, states, LANES), jnp.float32),
                pltpu.VMEM((Z, ne, spc, LANES), jnp.float32),
                pltpu.VMEM((max(Z - 1, 1), ne, spc, LANES), jnp.float32),
                pltpu.VMEM((R, ne, spc, LANES), jnp.float32),
                dma((2, 2)), dma, dma((units,)), dma((units,)), dma((units,)),
                dma((units,)), dma((units,)),
                dma((Z,)), dma((Z,)), dma((R,)), dma((R,)),
            ],
            compiler_params=pltpu.CompilerParams(
                collective_id=0, has_side_effects=True, vmem_limit_bytes=62 * 1024 * 1024),
            name="pole_sigma",
        )(frequency_grid, band_energy, eps_static, eps_imag,
          pair_elements.reshape(bpd * states, breadth))

    return jax.shard_map(
        shards,
        mesh=mesh,
        in_specs=(P("grow", "gcol"), P("grow", "gcol"), P(), P(), P("grow", None, "gcol")),
        out_specs=P(None, "gcol"),
        check_vma=False,
    )
```

```python
import functools

import jax
import jax.numpy as jnp
from jax import lax
from jax.experimental import pallas as pl
from jax.experimental.pallas import tpu as pltpu
from jax.sharding import PartitionSpec as P

LANES = 128
SUB_ROWS = 32
SUB_COLS = 512
DOT_COLS = 256


def bit_flip(index, mask, extent):
    total, bit = 0, 1
    while bit < extent:
        total = total + ((index // bit + mask // bit) % 2) * bit
        bit *= 2
    return total


def body(R, Z, bpd, states, height, breadth, ne,
         freq, energy, es_hbm, ei_hbm, pair_hbm, out,
         kern, colp, rowp, es_buf, ei_buf, sig, part, recv1, recv2, hold,
         eps_sem, own_sem, col_send, col_recv, row_recv, up_send, dn_send,
         s1_send, s1_recv, s2_send, s2_recv, hold_send, hold_recv, give_send):
    r = lax.axis_index("grow")
    z = lax.axis_index("gcol")
    ratio = R // Z
    home = r // ratio
    offset = pl.multiple_of(r % ratio * height, height)
    spc = states // Z
    units = R * bpd
    blocks = 4 * bpd
    rows = height // blocks

    def dev(row, col):
        return dict(device_id={"grow": row, "gcol": col}, device_id_type=pl.DeviceIdType.MESH)

    def eps_copies(block, slot):
        at = pl.multiple_of(block * rows, rows)
        return (pltpu.make_async_copy(es_hbm.at[pl.ds(at, rows), :], es_buf.at[slot], eps_sem.at[0, slot]),
                pltpu.make_async_copy(ei_hbm.at[pl.ds(at, rows), :], ei_buf.at[slot], eps_sem.at[1, slot]))

    own = pltpu.make_async_copy(pair_hbm, colp.at[0], own_sem)
    own.start()
    for copy in eps_copies(0, 0):
        copy.start()

    barrier = pltpu.get_barrier_semaphore()
    for d in range(1, R):
        pl.semaphore_signal(barrier, inc=1, **dev((r + d) % R, z))
    for d in range(1, Z):
        pl.semaphore_signal(barrier, inc=1, **dev(r, (z + d) % Z))
    sig[...] = jnp.zeros_like(sig)
    own.wait()
    pl.semaphore_wait(barrier, R + Z - 2)

    def unit_rows(b):
        return pl.ds(pl.multiple_of(b * states, states), states)

    def col_copy(src_shard, dst_shard, b, row):
        return pltpu.make_async_remote_copy(
            src_ref=colp.at[src_shard, unit_rows(b), :], dst_ref=colp.at[dst_shard, unit_rows(b), :],
            send_sem=col_send.at[dst_shard * bpd + b], recv_sem=col_recv.at[dst_shard * bpd + b],
            **dev(row, z))

    partner = bit_flip(r, 1, R)

    def send_own(b, carry):
        col_copy(0, 1, b, partner).start()
        return carry
    lax.fori_loop(0, bpd, send_own, 0)
    for shard in range(2, R, 2):
        peer = bit_flip(r, shard, R)

        def send_far(b, carry, shard=shard, peer=peer):
            col_copy(0, shard, b, peer).start()
            return carry
        lax.fori_loop(0, bpd, send_far, 0)

    def row_copy(shard, b, u, sems, col):
        ref = rowp.at[shard, unit_rows(b), :]
        return pltpu.make_async_remote_copy(
            src_ref=ref, dst_ref=ref, send_sem=sems.at[u], recv_sem=row_recv.at[u], **dev(r, col))

    side = bpd // 2
    keep = bpd - side
    items = (Z - 1) * side
    stride = 2 if 3 + 2 * (items - 1) < units else 1
    relay_down = home == 0
    relays = jnp.logical_or(relay_down, home == Z - 1)
    ahead = jnp.where(relay_down, z - 1, z + 1)
    has_ahead = jnp.logical_and(relays, jnp.logical_and(ahead >= 0, ahead < Z))
    ahead_col = (ahead + Z) % Z

    def side_copy(d, b):
        dst = hold.at[d, unit_rows(b), :]
        src = hold.at[d - 1, unit_rows(b), :] if not (isinstance(d, int) and d == 0) else colp.at[0, unit_rows(keep + b), :]
        return pltpu.make_async_remote_copy(
            src_ref=src, dst_ref=dst, send_sem=hold_send.at[d * side + b],
            recv_sem=hold_recv.at[d * side + b], **dev(r, ahead_col))

    def give_copy(d, b, k, panel):
        to = panel * ratio + k
        shard = bit_flip(r, to, R)
        return pltpu.make_async_remote_copy(
            src_ref=hold.at[d - 1, unit_rows(b), pl.ds(k * height, height)],
            dst_ref=rowp.at[shard, unit_rows(keep + b), :],
            send_sem=give_send.at[((d - 1) * side + b) * ratio + k],
            recv_sem=row_recv.at[shard * bpd + keep + b], **dev(to, z))

    def relay_item(t, act):
        d, b = t // side + 1, t % side
        panel = jnp.where(relay_down, z + d, z - d)

        @pl.when(jnp.logical_and(relays, jnp.logical_and(panel >= 0, panel < Z)))
        def _():
            act(d, b, (panel + Z) % Z)

    def pass_on(d, b, panel):
        pltpu.make_async_remote_copy(
            src_ref=hold.at[d - 1, unit_rows(b), :], dst_ref=hold.at[d - 1, unit_rows(b), :],
            send_sem=hold_send.at[(d - 1) * side + b], recv_sem=hold_recv.at[(d - 1) * side + b],
            **dev(r, ahead_col)).wait_recv()

        @pl.when(has_ahead)
        def _():
            side_copy(d, b).start()
        for k in range(ratio):
            give_copy(d, b, k, panel).start()

    def settle(d, b, panel):
        @pl.when(has_ahead)
        def _():
            side_copy(d, b).wait_send()
        for k in range(ratio):
            give_copy(d, b, k, panel).wait_send()

    @pl.when(has_ahead)
    def _():
        for b in range(side):
            side_copy(0, b).start()

    def aside(shard, b, group):
        return jnp.logical_and(b >= keep, bit_flip(r, shard, R) // ratio == group)

    goes_up = jnp.logical_and(z >= home, z < Z - 1)
    goes_down = jnp.logical_and(z <= home, z > 0)
    upper = (z + 1) % Z
    lower = (z + Z - 1) % Z

    def comm(u):
        shard, b = u // bpd, u % bpd

        @pl.when(shard >= 1)
        def _():
            col_copy(0, shard, b, partner).wait_recv()

        @pl.when(jnp.logical_and(shard >= 2, shard % 2 == 0))
        def _():
            col_copy(shard, shard + 1, b, partner).start()

        @pl.when(z == home)
        def _():
            local = pltpu.make_async_copy(
                colp.at[shard, unit_rows(b), pl.ds(offset, height)],
                rowp.at[shard, unit_rows(b), :], row_recv.at[u])
            local.start()
            local.wait()

        @pl.when(z != home)
        def _():
            row_copy(shard, b, u, up_send, upper).wait_recv()

        @pl.when(jnp.logical_and(goes_up, jnp.logical_not(aside(shard, b, Z - 1))))
        def _():
            row_copy(shard, b, u, up_send, upper).start()

        @pl.when(jnp.logical_and(goes_down, jnp.logical_not(aside(shard, b, 0))))
        def _():
            row_copy(shard, b, u, dn_send, lower).start()

        @pl.when(jnp.logical_and(jnp.logical_and(u >= 3, (u - 3) % stride == 0),
                                 (u - 3) // stride < items))
        def _():
            relay_item((u - 3) // stride, pass_on)

    diagonal = r * height - z * breadth
    sub_rows = min(SUB_ROWS, rows)
    sub_cols = min(SUB_COLS, breadth)
    col_steps = breadth // sub_cols
    f0, f1, f2 = freq[0], freq[1], freq[2]

    def make_block(block):
        slot = block % 2

        @pl.when(block + 1 < blocks)
        def _():
            for copy in eps_copies(block + 1, 1 - slot):
                copy.start()
        for copy in eps_copies(block, slot):
            copy.wait()
        base = pl.multiple_of(block * rows, rows)

        def chunk(n, carry):
            at_row = pl.multiple_of(n // col_steps * sub_rows, sub_rows)
            at_col = pl.multiple_of(n % col_steps * sub_cols, sub_cols)
            where = (pl.ds(at_row, sub_rows), pl.ds(at_col, sub_cols))
            gap = (lax.broadcasted_iota(jnp.int32, (sub_rows, sub_cols), 0)
                   - lax.broadcasted_iota(jnp.int32, (sub_rows, sub_cols), 1))
            one = jnp.where(gap == at_col - at_row - base - diagonal, 1.0, 0.0)
            static = es_buf[(slot,) + where] - one
            imag = ei_buf[(slot,) + where] - one
            spread = static - imag
            over = imag * imag + 0.25
            under = spread * spread + 0.25
            pole = over * lax.rsqrt(over * under)
            p0, p1, p2 = pole + f0, pole + f1, pole + f2
            p01 = p0 * p1
            scale = -static * pole / (p01 * p2)
            to = (pl.ds(pl.multiple_of(base + at_row, sub_rows), sub_rows), where[1])
            kern[(0,) + to] = (p1 * p2 * scale).astype(jnp.bfloat16)
            kern[(1,) + to] = (p0 * p2 * scale).astype(jnp.bfloat16)
            kern[(2,) + to] = (p01 * scale).astype(jnp.bfloat16)
            return carry
        lax.fori_loop(0, rows // sub_rows * col_steps, chunk, 0)

    width = breadth // bpd
    dot_cols = min(DOT_COLS, width)
    while width % dot_cols:
        dot_cols //= 2

    def piece(number):
        shard, q = number // bpd, number % bpd
        first = bit_flip(r, shard, R) * bpd

        def step(n, carry):
            cols = pl.ds(pl.multiple_of(q * width + n * dot_cols, dot_cols), dot_cols)
            right = colp[shard, :, cols].astype(jnp.float32)
            left = rowp[shard]
            sums = []
            for e in range(ne):
                prod = jnp.dot(left, kern[e, :, cols], preferred_element_type=jnp.float32) * right
                thin = prod[:, :LANES]
                for k in range(1, dot_cols // LANES):
                    thin = thin + prod[:, k * LANES:(k + 1) * LANES]
                total = carry[e]
                for b in range(bpd):
                    miss = jnp.full((8, LANES), freq[e] - energy[first + b], jnp.float32)
                    weight = (1.0 / (1.0 + miss * miss))[:1]
                    total = total + weight * thin[b * states:(b + 1) * states]
                sums.append(total)
            return tuple(sums)
        start = tuple(sig[e] for e in range(ne))
        done = lax.fori_loop(0, width // dot_cols, step, start)
        for e in range(ne):
            sig[e] = done[e]

    def phase_a(u, carry):
        comm(u)
        make_block(2 * u)
        make_block(2 * u + 1)
        return carry
    lax.fori_loop(0, 2 * bpd, phase_a, 0)

    def phase_b(u, carry):
        comm(u)
        piece(2 * (u - 2 * bpd))
        piece(2 * (u - 2 * bpd) + 1)
        return carry
    lax.fori_loop(2 * bpd, 3 * bpd, phase_b, 0)

    def phase_c(u, carry):
        comm(u)
        piece(u - bpd)
        return carry
    lax.fori_loop(3 * bpd, units, phase_c, 0)

    def phase_d(u, carry):
        piece(u - bpd)
        return carry
    lax.fori_loop(units, units + bpd, phase_d, 0)

    for owner in range(Z):
        for e in range(ne):
            part[owner, e] = sig[e, owner * spc:(owner + 1) * spc]

    def s1_copy(d):
        return pltpu.make_async_remote_copy(
            src_ref=part.at[(z + d) % Z], dst_ref=recv1.at[d - 1],
            send_sem=s1_send.at[d - 1], recv_sem=s1_recv.at[d - 1], **dev(r, (z + d) % Z))

    def s2_copy(d, owner):
        return pltpu.make_async_remote_copy(
            src_ref=recv2.at[owner], dst_ref=recv2.at[owner],
            send_sem=s2_send.at[d - 1], recv_sem=s2_recv.at[owner], **dev((r + d) % R, z))

    for d in range(1, Z):
        s1_copy(d).start()

    def drain(u, carry):
        shard, b = u // bpd, u % bpd

        @pl.when(shard >= 1)
        def _():
            col_copy(0, shard, b, partner).wait_send()

        @pl.when(jnp.logical_and(goes_up, jnp.logical_not(aside(shard, b, Z - 1))))
        def _():
            row_copy(shard, b, u, up_send, upper).wait_send()

        @pl.when(jnp.logical_and(goes_down, jnp.logical_not(aside(shard, b, 0))))
        def _():
            row_copy(shard, b, u, dn_send, lower).wait_send()
        return carry
    lax.fori_loop(0, units, drain, 0)

    @pl.when(has_ahead)
    def _():
        for b in range(side):
            side_copy(0, b).wait_send()

    def drain_side(t, carry):
        relay_item(t, settle)
        return carry
    lax.fori_loop(0, items, drain_side, 0)

    mine = part[z]
    for d in range(1, Z):
        s1_copy(d).wait_recv()
        mine = mine + recv1[d - 1]
    recv2[r] = mine
    for d in range(1, R):
        s2_copy(d, r).start()
    for d in range(1, R):
        s2_copy(d, (r + R - d) % R).wait_recv()
    full = recv2[0]
    for owner in range(1, R):
        full = full + recv2[owner]
    out[...] = jnp.sum(full, axis=-1)
    for d in range(1, Z):
        s1_copy(d).wait_send()
    for d in range(1, R):
        s2_copy(d, r).wait_send()


def solution(mesh):
    R, Z = mesh.shape["grow"], mesh.shape["gcol"]

    def shards(eps_static, eps_imag, frequency_grid, band_energy, pair_elements):
        height, breadth = eps_static.shape
        bpd, states, _ = pair_elements.shape
        ne = frequency_grid.shape[0]
        spc = states // Z
        rows = height // (4 * bpd)
        dma = pltpu.SemaphoreType.DMA
        units = R * bpd
        any_space = pl.BlockSpec(memory_space=pl.ANY)
        smem = pl.BlockSpec(memory_space=pltpu.SMEM)
        return pl.pallas_call(
            functools.partial(body, R, Z, bpd, states, height, breadth, ne),
            out_shape=jax.ShapeDtypeStruct((ne, spc), jnp.float32),
            in_specs=[smem, smem, any_space, any_space, any_space],
            out_specs=pl.BlockSpec(memory_space=pltpu.VMEM),
            scratch_shapes=[
                pltpu.VMEM((ne, height, breadth), jnp.bfloat16),
                pltpu.VMEM((R, bpd * states, breadth), jnp.bfloat16),
                pltpu.VMEM((R, bpd * states, height), jnp.bfloat16),
                pltpu.VMEM((2, rows, breadth), jnp.float32),
                pltpu.VMEM((2, rows, breadth), jnp.float32),
                pltpu.VMEM((ne, states, LANES), jnp.float32),
                pltpu.VMEM((Z, ne, spc, LANES), jnp.float32),
                pltpu.VMEM((max(Z - 1, 1), ne, spc, LANES), jnp.float32),
                pltpu.VMEM((R, ne, spc, LANES), jnp.float32),
                pltpu.VMEM((Z, bpd // 2 * states, breadth), jnp.bfloat16),
                dma((2, 2)), dma, dma((units,)), dma((units,)), dma((units,)),
                dma((units,)), dma((units,)),
                dma((Z,)), dma((Z,)), dma((R,)), dma((R,)),
                dma((Z * bpd,)), dma((Z * bpd,)), dma((Z * bpd * R // Z,)),
            ],
            compiler_params=pltpu.CompilerParams(
                collective_id=0, has_side_effects=True, vmem_limit_bytes=62 * 1024 * 1024),
            name="pole_sigma",
        )(frequency_grid, band_energy, eps_static, eps_imag,
          pair_elements.reshape(bpd * states, breadth))

    return jax.shard_map(
        shards,
        mesh=mesh,
        in_specs=(P("grow", "gcol"), P("grow", "gcol"), P(), P(), P("grow", None, "gcol")),
        out_specs=P(None, "gcol"),
        check_vma=False,
    )
```
